32 devices in a mesh: band: 4 (over x, core), fft: 8 (over z, y).
Axes of the slice: x: 2, y: 2, z: 4, core: 2. Of those that a mesh axis runs over, the one named last changes fastest.
Arguments:
- orbitals: bfloat16 [16, 2, 32768], P('band', None, 'fft'), may hold values from -6 to 6
- sphere_slot: int32 [32768], P('fft'), may hold values from 0 to 24575, as said below
- stick_column: int32 [1024], P('fft'), may hold values from 0 to 36863, as said below
- potential: float32 [192, 192, 192], P('fft'), may hold values from -3 to 3
- subspace: bfloat16 [64, 2, 32768], P('band', None, 'fft'), may hold values from -0.03125 to 0.03125
- previous: bfloat16 [16, 2, 32768], P('band', None, 'fft'), may hold values from -6 to 6
Outputs:
- applied: bfloat16 [16, 2, 32768], P('band', None, 'fft')
- intersection: float32 [2, 64, 16], P(None, 'fft', 'band')
The draws below stay inside these ranges and needn't reach their ends.
Inputs may be any that keep to these rules, and one draw needn't show every extreme that they name: `sphere_slot`: within each aligned block of 4096 entries the values are distinct. `stick_column`: aligned block d of 128 entries holds distinct columns x * 192 + y with d * 24 <= x < (d + 1) * 24.
All inputs are finite; a program needn't handle non-finite values.
Results may differ from the reference program's by a relative error of at most 0.012.
Values may be sent and summed in bfloat16 or wider, within the bound.
A program may use at most 64 MiB of HBM per device.

```python
import jax
import jax.numpy as jnp
from jax import lax

NG = 192
STK = 128
NPW_DEV = 4096
SUBB = 64
BANDS = 16
STICKS = 1024
NPW_TOT = 32768


def draw_sphere_slot(key, part):
    blocks = NPW_TOT // NPW_DEV
    keys = jax.random.split(jax.random.fold_in(key, 11), blocks)

    def one_block(block_key):
        return jax.random.permutation(block_key, NG * STK)[:NPW_DEV].astype(jnp.int32)
    return jax.vmap(one_block)(keys).reshape(-1).astype(jnp.int32)


def draw_stick_column(key, part):
    blocks = STICKS // STK
    slab_cells = NG // blocks * NG
    keys = jax.random.split(jax.random.fold_in(key, 23), blocks)

    def one_block(block_key, owner):
        return jax.random.permutation(block_key, slab_cells)[:STK].astype(jnp.int32) + owner * slab_cells
    owners = jnp.arange(blocks, dtype=jnp.int32)
    return jax.vmap(one_block)(keys, owners).reshape(-1).astype(jnp.int32)


def strengthened(result, rng, source, target, shards_of, factor):
    def block_of(axis_at):
        return (jnp.arange(result.shape[axis_at]) // (result.shape[axis_at] // shards_of)).reshape((-1,) + (1,) * (result.ndim - 1 - axis_at))

    first = jax.random.permutation(rng, shards_of)[block_of(target)]
    other_side = (block_of(target) + shards_of // 2) % shards_of
    return jnp.where((block_of(source) == first) | (block_of(source) == other_side), factor * result, result)


def level_of(stream_key, shape, cuts, low, high):
    factor_of, own = 1.0, jax.random.fold_in(stream_key, 6)
    for position, blocks in cuts:
        steps = jnp.exp(jax.random.uniform(jax.random.fold_in(own, position), (blocks,), jnp.float32, low / len(cuts), high / len(cuts)))
        factor_of = factor_of * jnp.repeat(steps, shape[position] // blocks).reshape([-1 if axis == position else 1 for axis in range(len(shape))])
    return factor_of


def scatter_about(own_key, extent, scale, reach, pieces=(), held_as=jnp.bfloat16):
    array = scale * jax.random.normal(own_key, extent, jnp.float32)
    if pieces:
        array = array * level_of(own_key, extent, pieces, -0.22, 0.18)
    return jnp.clip(array, -reach, reach).astype(held_as)


def bell_draw_with(rng, dims, scale, reach, cuts, heavy, kind=jnp.bfloat16):
    values = scale * jax.random.normal(rng, dims, jnp.float32)
    if cuts:
        values = values * level_of(rng, dims, cuts, -0.22, 0.18)
    return jnp.clip(strengthened(values, jax.random.fold_in(rng, 3), *heavy), -reach, reach).astype(kind)


def setup_inputs(seed: int = 0) -> dict:
    seeds = jax.random.split(jax.random.key(seed), 7)
    return {
        "orbitals": scatter_about(seeds[0], (BANDS, 2, NPW_TOT), 1.0, 6.0, ((0, 4), (2, 8))),
        "sphere_slot": draw_sphere_slot(jax.random.fold_in(seeds[6], 71), 0),
        "stick_column": draw_stick_column(jax.random.fold_in(seeds[6], 71), 0),
        "potential": jnp.clip(jax.random.uniform(seeds[3], (NG, NG, NG), jnp.float32, -3.0, 3.0) * level_of(seeds[3], (NG, NG, NG), ((0, 8),), -0.4, 0.0), -3.0, 3.0),
        "subspace": bell_draw_with(seeds[4], (SUBB, 2, NPW_TOT), (2 * NPW_TOT) ** -0.5, 0.03125, ((0, 4), (2, 8)), (2, 0, 8, 2.0)),
        "previous": scatter_about(seeds[5], (BANDS, 2, NPW_TOT), 1.0, 6.0, ((0, 4), (2, 8))),
    }


def frequency(values, grid_size):
    return jnp.where(values >= grid_size // 2, values - grid_size, values).astype(jnp.float32)


def rounded(values):
    real_part = lax.optimization_barrier(jnp.real(values).astype(jnp.bfloat16)).astype(jnp.float32)
    imag_part = lax.optimization_barrier(jnp.imag(values).astype(jnp.bfloat16)).astype(jnp.float32)
    return lax.complex(real_part, imag_part)


def reference(orbitals, sphere_slot, stick_column, potential, subspace, previous):
    owner = jnp.arange(NPW_TOT, dtype=jnp.int32) // NPW_DEV
    plane_index = (sphere_slot // STK).astype(jnp.int32)
    column = stick_column[(owner * STK + sphere_slot % STK).astype(jnp.int32)]
    cell = (plane_index * (NG * NG) + column).astype(jnp.int32)
    freq_z = frequency(plane_index, NG)
    freq_x = frequency(column // NG, NG)
    freq_y = frequency(column % NG, NG)
    kinetic = (freq_z * freq_z + freq_x * freq_x + freq_y * freq_y) * (2.0 / (NG * NG))

    def one_band(coeffs):
        real_in = coeffs[0].astype(jnp.float32)
        imag_in = coeffs[1].astype(jnp.float32)
        empty = jnp.zeros((NG * NG * NG,), jnp.float32)
        grid = lax.complex(empty.at[cell].set(real_in), empty.at[cell].set(imag_in)).reshape(NG, NG, NG)
        grid = rounded(jnp.fft.ifft(grid, axis=0, norm="forward"))
        grid = rounded(jnp.fft.ifft(grid, axis=2, norm="forward"))
        grid = rounded(jnp.fft.ifft(grid, axis=1, norm="forward") * potential)
        grid = rounded(jnp.fft.fft(grid, axis=1, norm="forward"))
        grid = rounded(jnp.fft.fft(grid, axis=2, norm="forward"))
        grid = jnp.fft.fft(grid, axis=0, norm="forward")
        values = grid.reshape(-1)[cell]
        applied_real = jnp.real(values) + kinetic * real_in
        applied_imag = jnp.imag(values) + kinetic * imag_in
        return jnp.stack([applied_real, applied_imag]).astype(jnp.bfloat16)

    applied = lax.map(one_band, orbitals)
    sub_real = subspace[:, 0]
    sub_imag = subspace[:, 1]
    prev_real = previous[:, 0]
    prev_imag = previous[:, 1]
    over_real = jnp.dot(sub_real, prev_real.T, preferred_element_type=jnp.float32) + jnp.dot(sub_imag, prev_imag.T, preferred_element_type=jnp.float32)
    over_imag = jnp.dot(sub_real, prev_imag.T, preferred_element_type=jnp.float32) - jnp.dot(sub_imag, prev_real.T, preferred_element_type=jnp.float32)
    return applied, jnp.stack([over_real, over_imag])
```

```python
import functools
import math

import jax
import jax.numpy as jnp
import numpy as np
from jax import lax
from jax.experimental import pallas as pl
from jax.experimental.pallas import tpu as pltpu
from jax.sharding import PartitionSpec as P


def dft_table(length, sign_value, factor):
    positions = jnp.arange(length, dtype=jnp.int32)
    phase_step = positions[:, None] * positions[None, :] % length
    angle_value = phase_step.astype(jnp.float32) * (2.0 * math.pi / length)
    cosine = (jnp.cos(angle_value) * factor).astype(jnp.bfloat16)
    sine_part = (jnp.sin(angle_value) * (sign_value * factor)).astype(jnp.bfloat16)
    return (cosine, sine_part)


def apply_dft(real_in, imag_in, table, form):
    cosine, sine_part = table

    def product(operand, table_part):
        return jnp.einsum(form, operand, table_part, preferred_element_type=jnp.float32)

    real_out = product(real_in, cosine) - product(imag_in, sine_part)
    imag_out = product(real_in, sine_part) + product(imag_in, cosine)
    return (real_out, imag_out)


def packed(pair, axis_pos):
    return jnp.stack([pair[0].astype(jnp.bfloat16), pair[1].astype(jnp.bfloat16)], axis=axis_pos)


def frequency(values, grid_size):
    return jnp.where(values >= grid_size // 2, values - grid_size, values).astype(jnp.float32)


def one_hot_rows(indices, count):
    return (indices[None, :] == jnp.arange(count, dtype=jnp.int32)[:, None]).astype(jnp.bfloat16)


def general_device(orbitals, sphere_slot, stick_column, potential, subspace, previous):
    slab_depth = potential.shape[0]
    grid_size = potential.shape[1]
    stick_count = stick_column.shape[0]
    slab_cells = slab_depth * grid_size
    forward = dft_table(grid_size, 1.0, 1.0)
    inverse = dft_table(grid_size, -1.0, 1.0 / grid_size)
    plane_index = sphere_slot // stick_count
    stick_index = sphere_slot % stick_count
    plane_hot = one_hot_rows(plane_index, grid_size)
    stick_hot = one_hot_rows(stick_index, stick_count)
    stick_coords = jnp.stack([stick_column // grid_size, stick_column % grid_size]).astype(
        jnp.bfloat16
    )
    wave_coords = jnp.dot(stick_coords, stick_hot, preferred_element_type=jnp.float32)
    freq_z = frequency(plane_index, grid_size)
    freq_x = frequency(wave_coords[0].astype(jnp.int32), grid_size)
    freq_y = frequency(wave_coords[1].astype(jnp.int32), grid_size)
    kinetic = (freq_z * freq_z + freq_x * freq_x + freq_y * freq_y) * (
        2.0 / (grid_size * grid_size)
    )
    prev_real = previous[:, 0]
    prev_imag = previous[:, 1]
    sub_piece = lax.all_gather(subspace, "band", axis=0, tiled=True)
    sub_real = sub_piece[:, 0]
    sub_imag = sub_piece[:, 1]
    over_real = jnp.einsum(
        "jg,ig->ji", sub_real, prev_real, preferred_element_type=jnp.float32
    ) + jnp.einsum("jg,ig->ji", sub_imag, prev_imag, preferred_element_type=jnp.float32)
    over_imag = jnp.einsum(
        "jg,ig->ji", sub_real, prev_imag, preferred_element_type=jnp.float32
    ) - jnp.einsum("jg,ig->ji", sub_imag, prev_real, preferred_element_type=jnp.float32)
    partial_value = jnp.stack([over_real, over_imag])
    intersection = lax.psum_scatter(partial_value, "fft", scatter_dimension=1, tiled=True)
    stick_buffer = jnp.einsum(
        "bpi,zi,si->bpzs", orbitals, plane_hot, stick_hot, preferred_element_type=jnp.float32
    ).astype(jnp.bfloat16)

    def potential_work(along_y):
        along_x = apply_dft(along_y[0], along_y[1], forward, "zxy,xk->zky")
        weighted = packed((along_x[0] * potential, along_x[1] * potential), 0)
        back_x = packed(apply_dft(weighted[0], weighted[1], inverse, "zxy,xk->zky"), 0)
        return packed(apply_dft(back_x[0], back_x[1], inverse, "zxy,yk->zxk"), 0)

    along_z = packed(apply_dft(stick_buffer[:, 0], stick_buffer[:, 1], forward, "bzs,zk->bks"), 1)
    all_columns = lax.all_gather(stick_column, "fft", axis=0, tiled=True)
    owners = all_columns.shape[0] // stick_count
    block_columns = (all_columns % slab_cells).reshape(owners, stick_count)
    block_hot = (
        block_columns[:, :, None] == jnp.arange(slab_cells, dtype=jnp.int32)[None, None, :]
    ).astype(jnp.bfloat16)

    def stick_work(one_band):
        plane_depth = one_band.shape[1]
        split_band = one_band.reshape(2, plane_depth, owners, stick_count)
        plane_grid = jnp.einsum(
            "pzds,dsc->pzdc", split_band, block_hot, preferred_element_type=jnp.float32
        ).astype(jnp.bfloat16)
        plane_grid = plane_grid.reshape(2, plane_depth, grid_size, grid_size)
        along_y = packed(apply_dft(plane_grid[0], plane_grid[1], forward, "zxy,yk->zxk"), 0)
        back_y = potential_work(along_y)
        back_split = back_y.reshape(2, plane_depth, owners, slab_cells)
        picked = jnp.einsum(
            "pzdc,dsc->pzds", back_split, block_hot, preferred_element_type=jnp.float32
        ).astype(jnp.bfloat16)
        return picked.reshape(2, plane_depth, owners * stick_count)

    finished = lax.map(
        stick_work, lax.all_to_all(along_z, "fft", split_axis=2, concat_axis=3, tiled=True)
    )
    stick_values = lax.all_to_all(finished, "fft", split_axis=3, concat_axis=2, tiled=True)
    picked_sticks = jnp.einsum(
        "bpzs,si->bpzi", stick_values, stick_hot, preferred_element_type=jnp.float32
    ).astype(jnp.bfloat16)
    cosine_cols = jnp.einsum("zk,ki->zi", inverse[0], plane_hot, preferred_element_type=jnp.float32)
    sine_cols = jnp.einsum("zk,ki->zi", inverse[1], plane_hot, preferred_element_type=jnp.float32)
    pick_real = picked_sticks[:, 0].astype(jnp.float32)
    pick_imag = picked_sticks[:, 1].astype(jnp.float32)
    wave_real = jnp.sum(pick_real * cosine_cols[None] - pick_imag * sine_cols[None], axis=1)
    wave_imag = jnp.sum(pick_real * sine_cols[None] + pick_imag * cosine_cols[None], axis=1)
    real_out = wave_real + kinetic * orbitals[:, 0].astype(jnp.float32)
    imag_out = wave_imag + kinetic * orbitals[:, 1].astype(jnp.float32)
    applied = jnp.stack([real_out, imag_out], axis=1).astype(jnp.bfloat16)
    return (applied, intersection)


PLANES = 4
EXTRA = 16


def phases(products, length):
    angle = (products % length).astype(np.float64) * (2.0 * np.pi / length)
    return np.cos(angle), np.sin(angle)


def line_tables(length):
    cosine, sine = phases(np.outer(np.arange(length), np.arange(length)), length)
    wide = -(-length // 128) * 128
    empty = np.zeros((length, wide - length))
    from_real = np.concatenate([cosine, empty, sine, empty], axis=1)
    from_imag = np.concatenate([-sine, empty, cosine, empty], axis=1)
    return jnp.asarray(np.stack([from_real, from_imag]), jnp.bfloat16)


def half_tables(length):
    half = np.arange(length // 2)
    tables = []
    for parity in (0, 1):
        cosine, sine = phases(np.outer(2 * half + parity, half), length)
        tables.append(np.block([[cosine, -sine], [sine, cosine]]))
    tables.extend([tables[0].T, tables[1].T])
    return jnp.asarray(np.stack(tables), jnp.bfloat16)


def plane_kernel(
    slab, stick_ref, pot_ref, line_ref, half_ref, out_ref, rows_ref, real_ref, imag_ref
):
    group = pl.program_id(0)
    owners, _, sticks = stick_ref.shape
    lines, size, _ = real_ref.shape
    half = size // 2
    wide = line_ref.shape[2] // 2
    part_rows = out_ref.shape[1] // 2
    first = pl.multiple_of(group * lines, lines)
    second = pl.multiple_of(part_rows + group * lines, lines)
    scale = 1.0 / (size * size)

    def stick_mask(owner):
        coords = stick_ref[owner, 2 * part_rows : 2 * part_rows + EXTRA, :].astype(jnp.float32)
        local = lax.broadcasted_iota(jnp.int32, (slab, sticks), 0).astype(jnp.float32)
        return coords[0:1, :] == local

    @pl.when(group == 0)
    def _():
        @pl.loop(0, owners)
        def _(owner):
            coords = stick_ref[owner, 2 * part_rows : 2 * part_rows + EXTRA, :].astype(jnp.float32)
            cells = lax.broadcasted_iota(jnp.int32, (size, sticks), 0).astype(jnp.float32)
            hot = jnp.where(coords[1:2, :] == cells, 1.0, 0.0).astype(jnp.bfloat16)
            for part in range(2):
                rows = lax.dot_general(
                    hot, line_ref[part], (((0,), (0,)), ((), ())),
                    preferred_element_type=jnp.float32,
                )
                rows_ref[owner, part * sticks : (part + 1) * sticks, :] = rows.astype(jnp.bfloat16)

    @pl.loop(0, owners)
    def _(owner):
        mask = stick_mask(owner)[None]
        spread = []
        for start in (first, second):
            values = stick_ref[owner, pl.ds(start, lines), :].astype(jnp.float32)
            spread.append(jnp.where(mask, values[:, None, :], 0.0).reshape(lines * slab, sticks))
        left = jnp.concatenate(spread, axis=1).astype(jnp.bfloat16)
        result = jnp.dot(left, rows_ref[owner], preferred_element_type=jnp.float32)
        place = pl.ds(pl.multiple_of(owner * slab, 8), slab)
        real_ref[:, place, :] = result[:, :size].reshape(lines, slab, size)
        imag_ref[:, place, :] = result[:, wide : wide + size].reshape(lines, slab, size)

    def one_plane(line, plane):
        real_low, real_high = real_ref[line, :half, :], real_ref[line, half:, :]
        imag_low, imag_high = imag_ref[line, :half, :], imag_ref[line, half:, :]
        total = jnp.concatenate([real_low + real_high, imag_low + imag_high], axis=0)
        differ = jnp.concatenate([real_low - real_high, imag_low - imag_high], axis=0)

        def there_and_back(values, parity):
            forward = jnp.dot(
                half_ref[parity], values.astype(jnp.bfloat16), preferred_element_type=jnp.float32
            )
            local = pot_ref[plane, parity]
            weighted = jnp.concatenate([forward[:half] * local, forward[half:] * local], axis=0)
            return jnp.dot(
                half_ref[2 + parity],
                weighted.astype(jnp.bfloat16),
                preferred_element_type=jnp.float32,
            )

        even = there_and_back(total, 0)
        odd = there_and_back(differ, 1)
        low, high = even + odd, even - odd
        real_ref[line, :half, :] = low[:half]
        imag_ref[line, :half, :] = low[half:]
        real_ref[line, half:, :] = high[:half]
        imag_ref[line, half:, :] = high[half:]

    bands = lines // PLANES

    @pl.loop(0, PLANES)
    def _(plane):
        for band in range(bands):
            one_plane(plane * bands + band, plane)

    @pl.loop(0, owners)
    def _(owner):
        mask = stick_mask(owner)[None]
        place = pl.ds(pl.multiple_of(owner * slab, 8), slab)
        real = real_ref[:, place, :].reshape(lines * slab, size).astype(jnp.bfloat16)
        imag = imag_ref[:, place, :].reshape(lines * slab, size).astype(jnp.bfloat16)
        across = (((1,), (1,)), ((), ()))
        result = lax.dot_general(
            real, rows_ref[owner, :, :size], across, preferred_element_type=jnp.float32
        ) + lax.dot_general(
            imag, rows_ref[owner, :, wide : wide + size], across, preferred_element_type=jnp.float32
        )
        result = result.reshape(lines, slab, 2 * sticks)
        for part, start in enumerate((first, second)):
            chosen = result[:, :, part * sticks : (part + 1) * sticks]
            picked = jnp.sum(jnp.where(mask, chosen, 0.0), axis=1) * scale
            out_ref[owner, pl.ds(start, lines), :] = picked.astype(jnp.bfloat16)


def plane_work(received, potential, bands):
    owners, _, sticks = received.shape
    slab, size, _ = potential.shape
    lines = PLANES * bands
    split_pot = potential.reshape(slab, size // 2, 2, size).transpose(0, 2, 1, 3)
    lines_table = line_tables(size)
    halves = half_tables(size)
    wide = lines_table.shape[2]

    def whole(array):
        return pl.BlockSpec(array.shape, lambda g: (0,) * array.ndim)

    rows = 2 * slab * bands
    return pl.pallas_call(
        lambda *refs: plane_kernel(slab, *refs),
        grid=(slab // PLANES,),
        out_shape=jax.ShapeDtypeStruct((owners, rows, sticks), jnp.bfloat16),
        in_specs=[
            whole(received),
            pl.BlockSpec((PLANES, 2, size // 2, size), lambda g: (g, 0, 0, 0)),
            whole(lines_table),
            whole(halves),
        ],
        out_specs=pl.BlockSpec((owners, rows, sticks), lambda g: (0, 0, 0)),
        scratch_shapes=[
            pltpu.VMEM((owners, 2 * sticks, wide), jnp.bfloat16),
            pltpu.VMEM((lines, size, size), jnp.float32),
            pltpu.VMEM((lines, size, size), jnp.float32),
        ],
        compiler_params=pltpu.CompilerParams(
            dimension_semantics=("arbitrary",), vmem_limit_bytes=48 * 1024 * 1024
        ),
        cost_estimate=pl.CostEstimate(
            flops=40 * 10**9, bytes_accessed=8 * 10**6, transcendentals=0
        ),
    )(received, split_pot, lines_table, halves)


def gathered_bands(array, mesh_bands):
    here = lax.axis_index("band")
    blocks = [array]
    for shift in range(1, mesh_bands):
        pairs = [((src + shift) % mesh_bands, src) for src in range(mesh_bands)]
        blocks.append(lax.ppermute(array, "band", pairs))
    return blocks, here


def overlaps(subspace, previous, mesh_bands, owners):
    blocks, here = gathered_bands(subspace, mesh_bands)
    prev_real, prev_imag = previous[:, 0], previous[:, 1]
    right = jnp.concatenate(
        [
            jnp.concatenate([prev_real, prev_imag], axis=1),
            jnp.concatenate([prev_imag, -prev_real], axis=1),
        ],
        axis=0,
    )
    partials = []
    for block in blocks:
        partials.append(
            jnp.einsum(
                "jg,ig->ji",
                block.reshape(block.shape[0], -1),
                right,
                preferred_element_type=jnp.float32,
            )
        )
    twice = jnp.concatenate(partials + partials, axis=0)
    count = twice.shape[0] // 2
    start = (count - here * subspace.shape[0]) % count
    ordered = lax.dynamic_slice_in_dim(twice, start, count, axis=0)
    split = ordered.reshape(owners, count // owners, 2, previous.shape[0])
    return split.transpose(0, 2, 1, 3)


def fast_device(mesh_bands, orbitals, sphere_slot, stick_column, potential, subspace, previous):
    slab_depth, grid_size, _ = potential.shape
    stick_count = stick_column.shape[0]
    owners = grid_size // slab_depth
    bands = orbitals.shape[0]
    forward = dft_table(grid_size, 1.0, 1.0)
    inverse = dft_table(grid_size, -1.0, 1.0 / grid_size)
    plane_index = sphere_slot // stick_count
    stick_index = sphere_slot % stick_count
    plane_hot = one_hot_rows(plane_index, grid_size)
    stick_hot = one_hot_rows(stick_index, stick_count)
    stick_x = stick_column // grid_size
    stick_y = stick_column % grid_size
    stick_coords = jnp.stack([stick_x, stick_y]).astype(jnp.bfloat16)
    wave_coords = jnp.dot(stick_coords, stick_hot, preferred_element_type=jnp.float32)
    freq_z = frequency(plane_index, grid_size)
    freq_x = frequency(wave_coords[0].astype(jnp.int32), grid_size)
    freq_y = frequency(wave_coords[1].astype(jnp.int32), grid_size)
    kinetic = (freq_z * freq_z + freq_x * freq_x + freq_y * freq_y) * (
        2.0 / (grid_size * grid_size)
    )
    local_x = stick_x - lax.axis_index("fft") * slab_depth
    coords = jnp.stack([local_x, stick_y]).astype(jnp.bfloat16)
    coords = jnp.pad(coords, ((0, EXTRA - 2), (0, 0)))
    coords = jnp.broadcast_to(coords[None], (owners, EXTRA, stick_count))
    stick_buffer = jnp.einsum(
        "bpi,zi,si->pzbs", orbitals, plane_hot, stick_hot, preferred_element_type=jnp.float32
    ).astype(jnp.bfloat16)
    along_z = apply_dft(stick_buffer[0], stick_buffer[1], forward, "zbs,zk->kbs")
    pieces = [part.astype(jnp.bfloat16).reshape(owners, -1, stick_count) for part in along_z]
    sent = jnp.concatenate(pieces + [coords], axis=1)
    received = lax.all_to_all(sent, "fft", split_axis=0, concat_axis=0, tiled=True)
    planes = plane_work(received, potential, bands)
    split = overlaps(subspace, previous, mesh_bands, owners)
    flat = split.reshape(owners, 1, -1)
    high = lax.reduce_precision(flat, 8, 7)
    low = lax.reduce_precision(flat - high, 8, 7)
    both = jnp.concatenate([high, low], axis=2).astype(jnp.bfloat16)
    width = both.shape[2]
    lanes = -(-width // stick_count) * stick_count
    both = jnp.pad(both, ((0, 0), (0, 0), (0, lanes - width)))
    both = both.reshape(owners, -1, stick_count)
    both = jnp.pad(both, ((0, 0), (0, EXTRA - both.shape[1]), (0, 0)))
    returned = lax.all_to_all(
        jnp.concatenate([planes, both], axis=1), "fft", split_axis=0, concat_axis=0, tiled=True
    )
    rows = planes.shape[1]
    sums = returned[:, rows:].reshape(owners, -1)[:, :width].astype(jnp.float32)
    sums = jnp.sum(sums, axis=0)
    intersection = (sums[: width // 2] + sums[width // 2 :]).reshape(split.shape[1:])
    stick_values = returned[:, :rows].reshape(owners, 2, slab_depth, bands, stick_count)
    picked = jnp.einsum(
        "dpzbs,si->pdzbi", stick_values, stick_hot, preferred_element_type=jnp.float32
    ).astype(jnp.bfloat16)
    picked = picked.reshape(2, grid_size, bands, -1)
    cosine_cols = jnp.einsum("zk,ki->zi", inverse[0], plane_hot, preferred_element_type=jnp.float32)
    sine_cols = jnp.einsum("zk,ki->zi", inverse[1], plane_hot, preferred_element_type=jnp.float32)
    pick_real = picked[0].astype(jnp.float32)
    pick_imag = picked[1].astype(jnp.float32)
    cosine_cols = cosine_cols[:, None]
    sine_cols = sine_cols[:, None]
    wave_real = jnp.sum(pick_real * cosine_cols - pick_imag * sine_cols, axis=0)
    wave_imag = jnp.sum(pick_real * sine_cols + pick_imag * cosine_cols, axis=0)
    real_out = wave_real + kinetic * orbitals[:, 0].astype(jnp.float32)
    imag_out = wave_imag + kinetic * orbitals[:, 1].astype(jnp.float32)
    applied = jnp.stack([real_out, imag_out], axis=1).astype(jnp.bfloat16)
    return (applied, intersection)


def per_device(mesh_bands, *arrays):
    orbitals, _, _, potential, _, previous = arrays
    slab_depth = potential.shape[0]
    bands = orbitals.shape[0]
    aligned = slab_depth % 8 == 0 and slab_depth % PLANES == 0
    if aligned and PLANES * bands % 16 == 0 and arrays[2].shape[0] % 128 == 0:
        return fast_device(mesh_bands, *arrays)
    return general_device(*arrays)


def solution(mesh):
    return jax.shard_map(
        functools.partial(per_device, mesh.shape["band"]),
        mesh=mesh,
        in_specs=(
            P("band", None, "fft"),
            P("fft"),
            P("fft"),
            P("fft", None, None),
            P("band", None, "fft"),
            P("band", None, "fft"),
        ),
        out_specs=(P("band", None, "fft"), P(None, "fft", "band")),
        check_vma=False,
    )
```

```python
import functools
import math

import jax
import jax.numpy as jnp
import numpy as np
from jax import lax
from jax.experimental import pallas as pl
from jax.experimental.pallas import tpu as pltpu
from jax.sharding import PartitionSpec as P


def dft_table(length, sign_value, factor):
    positions = jnp.arange(length, dtype=jnp.int32)
    phase_step = positions[:, None] * positions[None, :] % length
    angle_value = phase_step.astype(jnp.float32) * (2.0 * math.pi / length)
    cosine = (jnp.cos(angle_value) * factor).astype(jnp.bfloat16)
    sine_part = (jnp.sin(angle_value) * (sign_value * factor)).astype(jnp.bfloat16)
    return (cosine, sine_part)


def apply_dft(real_in, imag_in, table, form):
    cosine, sine_part = table

    def product(operand, table_part):
        return jnp.einsum(form, operand, table_part, preferred_element_type=jnp.float32)

    real_out = product(real_in, cosine) - product(imag_in, sine_part)
    imag_out = product(real_in, sine_part) + product(imag_in, cosine)
    return (real_out, imag_out)


def packed(pair, axis_pos):
    return jnp.stack([pair[0].astype(jnp.bfloat16), pair[1].astype(jnp.bfloat16)], axis=axis_pos)


def frequency(values, grid_size):
    return jnp.where(values >= grid_size // 2, values - grid_size, values).astype(jnp.float32)


def one_hot_rows(indices, count):
    return (indices[None, :] == jnp.arange(count, dtype=jnp.int32)[:, None]).astype(jnp.bfloat16)


def general_device(orbitals, sphere_slot, stick_column, potential, subspace, previous):
    slab_depth = potential.shape[0]
    grid_size = potential.shape[1]
    stick_count = stick_column.shape[0]
    slab_cells = slab_depth * grid_size
    forward = dft_table(grid_size, 1.0, 1.0)
    inverse = dft_table(grid_size, -1.0, 1.0 / grid_size)
    plane_index = sphere_slot // stick_count
    stick_index = sphere_slot % stick_count
    plane_hot = one_hot_rows(plane_index, grid_size)
    stick_hot = one_hot_rows(stick_index, stick_count)
    stick_coords = jnp.stack([stick_column // grid_size, stick_column % grid_size]).astype(
        jnp.bfloat16
    )
    wave_coords = jnp.dot(stick_coords, stick_hot, preferred_element_type=jnp.float32)
    freq_z = frequency(plane_index, grid_size)
    freq_x = frequency(wave_coords[0].astype(jnp.int32), grid_size)
    freq_y = frequency(wave_coords[1].astype(jnp.int32), grid_size)
    kinetic = (freq_z * freq_z + freq_x * freq_x + freq_y * freq_y) * (
        2.0 / (grid_size * grid_size)
    )
    prev_real = previous[:, 0]
    prev_imag = previous[:, 1]
    sub_piece = lax.all_gather(subspace, "band", axis=0, tiled=True)
    sub_real = sub_piece[:, 0]
    sub_imag = sub_piece[:, 1]
    over_real = jnp.einsum(
        "jg,ig->ji", sub_real, prev_real, preferred_element_type=jnp.float32
    ) + jnp.einsum("jg,ig->ji", sub_imag, prev_imag, preferred_element_type=jnp.float32)
    over_imag = jnp.einsum(
        "jg,ig->ji", sub_real, prev_imag, preferred_element_type=jnp.float32
    ) - jnp.einsum("jg,ig->ji", sub_imag, prev_real, preferred_element_type=jnp.float32)
    partial_value = jnp.stack([over_real, over_imag])
    intersection = lax.psum_scatter(partial_value, "fft", scatter_dimension=1, tiled=True)
    stick_buffer = jnp.einsum(
        "bpi,zi,si->bpzs", orbitals, plane_hot, stick_hot, preferred_element_type=jnp.float32
    ).astype(jnp.bfloat16)

    def potential_work(along_y):
        along_x = apply_dft(along_y[0], along_y[1], forward, "zxy,xk->zky")
        weighted = packed((along_x[0] * potential, along_x[1] * potential), 0)
        back_x = packed(apply_dft(weighted[0], weighted[1], inverse, "zxy,xk->zky"), 0)
        return packed(apply_dft(back_x[0], back_x[1], inverse, "zxy,yk->zxk"), 0)

    along_z = packed(apply_dft(stick_buffer[:, 0], stick_buffer[:, 1], forward, "bzs,zk->bks"), 1)
    all_columns = lax.all_gather(stick_column, "fft", axis=0, tiled=True)
    owners = all_columns.shape[0] // stick_count
    block_columns = (all_columns % slab_cells).reshape(owners, stick_count)
    block_hot = (
        block_columns[:, :, None] == jnp.arange(slab_cells, dtype=jnp.int32)[None, None, :]
    ).astype(jnp.bfloat16)

    def stick_work(one_band):
        plane_depth = one_band.shape[1]
        split_band = one_band.reshape(2, plane_depth, owners, stick_count)
        plane_grid = jnp.einsum(
            "pzds,dsc->pzdc", split_band, block_hot, preferred_element_type=jnp.float32
        ).astype(jnp.bfloat16)
        plane_grid = plane_grid.reshape(2, plane_depth, grid_size, grid_size)
        along_y = packed(apply_dft(plane_grid[0], plane_grid[1], forward, "zxy,yk->zxk"), 0)
        back_y = potential_work(along_y)
        back_split = back_y.reshape(2, plane_depth, owners, slab_cells)
        picked = jnp.einsum(
            "pzdc,dsc->pzds", back_split, block_hot, preferred_element_type=jnp.float32
        ).astype(jnp.bfloat16)
        return picked.reshape(2, plane_depth, owners * stick_count)

    finished = lax.map(
        stick_work, lax.all_to_all(along_z, "fft", split_axis=2, concat_axis=3, tiled=True)
    )
    stick_values = lax.all_to_all(finished, "fft", split_axis=3, concat_axis=2, tiled=True)
    picked_sticks = jnp.einsum(
        "bpzs,si->bpzi", stick_values, stick_hot, preferred_element_type=jnp.float32
    ).astype(jnp.bfloat16)
    cosine_cols = jnp.einsum("zk,ki->zi", inverse[0], plane_hot, preferred_element_type=jnp.float32)
    sine_cols = jnp.einsum("zk,ki->zi", inverse[1], plane_hot, preferred_element_type=jnp.float32)
    pick_real = picked_sticks[:, 0].astype(jnp.float32)
    pick_imag = picked_sticks[:, 1].astype(jnp.float32)
    wave_real = jnp.sum(pick_real * cosine_cols[None] - pick_imag * sine_cols[None], axis=1)
    wave_imag = jnp.sum(pick_real * sine_cols[None] + pick_imag * cosine_cols[None], axis=1)
    real_out = wave_real + kinetic * orbitals[:, 0].astype(jnp.float32)
    imag_out = wave_imag + kinetic * orbitals[:, 1].astype(jnp.float32)
    applied = jnp.stack([real_out, imag_out], axis=1).astype(jnp.bfloat16)
    return (applied, intersection)


PLANES = 4
EXTRA = 16
LANES = 128


def phases(products, length):
    angle = (products % length).astype(np.float64) * (2.0 * np.pi / length)
    return np.cos(angle), np.sin(angle)


def line_tables(length):
    cosine, sine = phases(np.outer(np.arange(length), np.arange(length)), length)
    wide = -(-length // 128) * 128
    empty = np.zeros((length, wide - length))
    from_real = np.concatenate([cosine, empty, sine, empty], axis=1)
    from_imag = np.concatenate([-sine, empty, cosine, empty], axis=1)
    return jnp.asarray(np.stack([from_real, from_imag]), jnp.bfloat16)


def half_tables(length):
    half = np.arange(length // 2)
    tables = []
    for parity in (0, 1):
        cosine, sine = phases(np.outer(2 * half + parity, half), length)
        tables.append(np.block([[cosine, -sine], [sine, cosine]]))
    tables.extend([tables[0].T, tables[1].T])
    return jnp.asarray(np.stack(tables), jnp.bfloat16)


def plane_kernel(
    slab,
    stick_ref,
    pot_ref,
    line_ref,
    half_ref,
    extra_ref,
    back_ref,
    rows_ref,
    real_ref,
    imag_ref,
    after_real_ref,
    after_imag_ref,
    left_ref,
    right_ref,
    stage_ref,
    send_sem,
    recv_sem,
):
    owners, _, sticks = stick_ref.shape
    lines, size, _ = real_ref.shape
    half = size // 2
    wide = line_ref.shape[2] // 2
    groups = slab // PLANES
    part_rows = groups * lines
    me = lax.axis_index("fft")
    others = [lax.rem(me + shift, owners) for shift in range(1, owners)]
    scale = 1.0 / (size * size)

    def stick_mask(owner):
        coords = stick_ref[owner, 2 * part_rows : 2 * part_rows + EXTRA, :].astype(jnp.float32)
        local = lax.broadcasted_iota(jnp.int32, (slab, sticks), 0).astype(jnp.float32)
        return coords[0:1, :] == local

    def plane_group(group):
        first = pl.multiple_of(group * lines, lines)
        second = pl.multiple_of(part_rows + group * lines, lines)

        @pl.loop(0, owners, unroll=2)
        def _(owner):
            mask = stick_mask(owner)[None]
            spread = []
            for start in (first, second):
                values = stick_ref[owner, pl.ds(start, lines), :].astype(jnp.float32)
                spread.append(
                    jnp.where(mask, values[:, None, :], 0.0).reshape(lines * slab, sticks)
                )
            left = jnp.concatenate(spread, axis=1).astype(jnp.bfloat16)
            result = jnp.dot(left, rows_ref[owner], preferred_element_type=jnp.float32)
            place = pl.ds(pl.multiple_of(owner * slab, 8), slab)
            real_ref[:, place, :] = result[:, :size].reshape(lines, slab, size)
            imag_ref[:, place, :] = result[:, wide : wide + size].reshape(lines, slab, size)

        def one_plane(line, plane):
            real_low, real_high = real_ref[line, :half, :], real_ref[line, half:, :]
            imag_low, imag_high = imag_ref[line, :half, :], imag_ref[line, half:, :]
            total = jnp.concatenate([real_low + real_high, imag_low + imag_high], axis=0)
            differ = jnp.concatenate([real_low - real_high, imag_low - imag_high], axis=0)

            def there_and_back(values, parity):
                forward = jnp.dot(
                    half_ref[parity],
                    values.astype(jnp.bfloat16),
                    preferred_element_type=jnp.float32,
                )
                picks = pl.ds(parity, half, 2)
                local = jnp.concatenate(
                    [left_ref[plane, picks, :], right_ref[plane, picks, :][:, : size - LANES]], axis=1
                )
                weighted = jnp.concatenate([forward[:half] * local, forward[half:] * local], axis=0)
                return jnp.dot(
                    half_ref[2 + parity],
                    weighted.astype(jnp.bfloat16),
                    preferred_element_type=jnp.float32,
                )

            even = there_and_back(total, 0)
            odd = there_and_back(differ, 1)
            low, high = even + odd, even - odd
            after_real_ref[line, :half, :] = low[:half]
            after_imag_ref[line, :half, :] = low[half:]
            after_real_ref[line, half:, :] = high[:half]
            after_imag_ref[line, half:, :] = high[half:]

        bands = lines // PLANES

        @pl.loop(0, PLANES)
        def _(plane):
            whole_plane = group * PLANES + plane
            left_ref[plane] = pot_ref[whole_plane, :, :LANES]
            right_ref[plane, :, : size - LANES] = pot_ref[whole_plane, :, LANES:]
            for band in range(bands):
                one_plane(plane * bands + band, plane)

        @pl.loop(0, owners, unroll=2)
        def _(owner):
            mask = stick_mask(owner)[None]
            place = pl.ds(pl.multiple_of(owner * slab, 8), slab)
            real = after_real_ref[:, place, :].reshape(lines * slab, size).astype(jnp.bfloat16)
            imag = after_imag_ref[:, place, :].reshape(lines * slab, size).astype(jnp.bfloat16)
            across = (((1,), (1,)), ((), ()))
            result = lax.dot_general(
                real, rows_ref[owner, :, :size], across, preferred_element_type=jnp.float32
            ) + lax.dot_general(
                imag,
                rows_ref[owner, :, wide : wide + size],
                across,
                preferred_element_type=jnp.float32,
            )
            result = result.reshape(lines, slab, 2 * sticks)
            for part in range(2):
                chosen = result[:, :, part * sticks : (part + 1) * sticks]
                picked = jnp.sum(jnp.where(mask, chosen, 0.0), axis=1) * scale
                start = pl.multiple_of((2 * group + part) * lines, lines)
                stage_ref[owner, pl.ds(start, lines), :] = picked.astype(jnp.bfloat16)

    def rows_of(group):
        return pl.ds(pl.multiple_of(group * 2 * lines, 2 * lines), 2 * lines)

    def group_copy(group, place):
        return pltpu.make_async_remote_copy(
            src_ref=stage_ref.at[others[place], rows_of(group)],
            dst_ref=back_ref.at[me, rows_of(group)],
            send_sem=send_sem.at[group, place],
            recv_sem=recv_sem.at[group, place],
            device_id={"fft": others[place]},
            device_id_type=pl.DeviceIdType.MESH,
        )

    def extra_copy(place):
        return pltpu.make_async_remote_copy(
            src_ref=extra_ref.at[others[place]],
            dst_ref=back_ref.at[me, pl.ds(2 * part_rows, EXTRA)],
            send_sem=send_sem.at[groups, place],
            recv_sem=recv_sem.at[groups, place],
            device_id={"fft": others[place]},
            device_id_type=pl.DeviceIdType.MESH,
        )

    barrier = pltpu.get_barrier_semaphore()
    for other in others:
        pl.semaphore_signal(
            barrier, inc=1, device_id={"fft": other}, device_id_type=pl.DeviceIdType.MESH
        )

    @pl.loop(0, owners)
    def _(owner):
        coords = stick_ref[owner, 2 * part_rows : 2 * part_rows + EXTRA, :].astype(jnp.float32)
        cells = lax.broadcasted_iota(jnp.int32, (size, sticks), 0).astype(jnp.float32)
        hot = jnp.where(coords[1:2, :] == cells, 1.0, 0.0).astype(jnp.bfloat16)
        for part in range(2):
            rows = lax.dot_general(
                hot,
                line_ref[part],
                (((0,), (0,)), ((), ())),
                preferred_element_type=jnp.float32,
            )
            rows_ref[owner, part * sticks : (part + 1) * sticks, :] = rows.astype(jnp.bfloat16)

    pl.semaphore_wait(barrier, owners - 1)
    for place in range(owners - 1):
        extra_copy(place).start()

    @pl.loop(0, groups)
    def _(group):
        plane_group(group)
        for place in range(owners - 1):
            group_copy(group, place).start()

    back_ref[me, : 2 * part_rows, :] = stage_ref[me]
    back_ref[me, 2 * part_rows :, :] = extra_ref[me]
    for place in range(owners - 1):
        extra_copy(place).wait()

    @pl.loop(0, groups)
    def _(group):
        for place in range(owners - 1):
            group_copy(group, place).wait()


def plane_work(received, potential, extra, bands):
    owners, _, sticks = received.shape
    slab, size, _ = potential.shape
    lines = PLANES * bands
    groups = slab // PLANES
    lines_table = line_tables(size)
    halves = half_tables(size)
    wide = lines_table.shape[2]
    rows = 2 * slab * bands
    in_vmem = pl.BlockSpec(memory_space=pltpu.VMEM)
    grid_part = pltpu.VMEM((lines, size, size), jnp.float32)
    return pl.pallas_call(
        functools.partial(plane_kernel, slab),
        out_shape=jax.ShapeDtypeStruct((owners, rows + EXTRA, sticks), jnp.bfloat16),
        in_specs=[in_vmem] * 5,
        out_specs=in_vmem,
        scratch_shapes=[
            pltpu.VMEM((owners, 2 * sticks, wide), jnp.bfloat16),
            grid_part,
            grid_part,
            grid_part,
            grid_part,
            pltpu.VMEM((PLANES, size, LANES), jnp.float32),
            pltpu.VMEM((PLANES, size, LANES), jnp.float32),
            pltpu.VMEM((owners, rows, sticks), jnp.bfloat16),
            pltpu.SemaphoreType.DMA((groups + 1, owners - 1)),
            pltpu.SemaphoreType.DMA((groups + 1, owners - 1)),
        ],
        compiler_params=pltpu.CompilerParams(
            collective_id=0, has_side_effects=True, vmem_limit_bytes=48 * 1024 * 1024
        ),
        cost_estimate=pl.CostEstimate(
            flops=40 * 10**9, bytes_accessed=8 * 10**6, transcendentals=0
        ),
    )(received, potential, lines_table, halves, extra)


def gathered_bands(array, mesh_bands):
    here = lax.axis_index("band")
    blocks = [array]
    for shift in range(1, mesh_bands):
        pairs = [((src + shift) % mesh_bands, src) for src in range(mesh_bands)]
        blocks.append(lax.ppermute(array, "band", pairs))
    return blocks, here


def overlaps(subspace, previous, mesh_bands, owners):
    blocks, here = gathered_bands(subspace, mesh_bands)
    prev_real, prev_imag = previous[:, 0], previous[:, 1]
    right = jnp.concatenate(
        [
            jnp.concatenate([prev_real, prev_imag], axis=1),
            jnp.concatenate([prev_imag, -prev_real], axis=1),
        ],
        axis=0,
    )
    partials = []
    for block in blocks:
        partials.append(
            jnp.einsum(
                "jg,ig->ji",
                block.reshape(block.shape[0], -1),
                right,
                preferred_element_type=jnp.float32,
            )
        )
    twice = jnp.concatenate(partials + partials, axis=0)
    count = twice.shape[0] // 2
    start = (count - here * subspace.shape[0]) % count
    ordered = lax.dynamic_slice_in_dim(twice, start, count, axis=0)
    split = ordered.reshape(owners, count // owners, 2, previous.shape[0])
    return split.transpose(0, 2, 1, 3)


def fast_device(mesh_bands, orbitals, sphere_slot, stick_column, potential, subspace, previous):
    slab_depth, grid_size, _ = potential.shape
    stick_count = stick_column.shape[0]
    owners = grid_size // slab_depth
    bands = orbitals.shape[0]
    forward = dft_table(grid_size, 1.0, 1.0)
    inverse = dft_table(grid_size, -1.0, 1.0 / grid_size)
    plane_index = sphere_slot // stick_count
    stick_index = sphere_slot % stick_count
    plane_hot = one_hot_rows(plane_index, grid_size)
    stick_hot = one_hot_rows(stick_index, stick_count)
    stick_x = stick_column // grid_size
    stick_y = stick_column % grid_size
    stick_coords = jnp.stack([stick_x, stick_y]).astype(jnp.bfloat16)
    wave_coords = jnp.dot(stick_coords, stick_hot, preferred_element_type=jnp.float32)
    freq_z = frequency(plane_index, grid_size)
    freq_x = frequency(wave_coords[0].astype(jnp.int32), grid_size)
    freq_y = frequency(wave_coords[1].astype(jnp.int32), grid_size)
    kinetic = (freq_z * freq_z + freq_x * freq_x + freq_y * freq_y) * (
        2.0 / (grid_size * grid_size)
    )
    local_x = stick_x - lax.axis_index("fft") * slab_depth
    coords = jnp.stack([local_x, stick_y]).astype(jnp.bfloat16)
    coords = jnp.pad(coords, ((0, EXTRA - 2), (0, 0)))
    coords = jnp.broadcast_to(coords[None], (owners, EXTRA, stick_count))
    stick_buffer = jnp.einsum(
        "bpi,zi,si->pzbs", orbitals, plane_hot, stick_hot, preferred_element_type=jnp.float32
    ).astype(jnp.bfloat16)
    along_z = apply_dft(stick_buffer[0], stick_buffer[1], forward, "zbs,zk->kbs")
    pieces = [part.astype(jnp.bfloat16).reshape(owners, -1, stick_count) for part in along_z]
    sent = jnp.concatenate(pieces + [coords], axis=1)
    received = lax.all_to_all(sent, "fft", split_axis=0, concat_axis=0, tiled=True)
    split = overlaps(subspace, previous, mesh_bands, owners)
    flat = split.reshape(owners, 1, -1)
    high = lax.reduce_precision(flat, 8, 7)
    low = lax.reduce_precision(flat - high, 8, 7)
    both = jnp.concatenate([high, low], axis=2).astype(jnp.bfloat16)
    width = both.shape[2]
    lanes = -(-width // stick_count) * stick_count
    both = jnp.pad(both, ((0, 0), (0, 0), (0, lanes - width)))
    both = both.reshape(owners, -1, stick_count)
    both = jnp.pad(both, ((0, 0), (0, EXTRA - both.shape[1]), (0, 0)))
    returned = plane_work(received, potential, both, bands)
    rows = 2 * slab_depth * bands
    sums = returned[:, rows:].reshape(owners, -1)[:, :width].astype(jnp.float32)
    sums = jnp.sum(sums, axis=0)
    intersection = (sums[: width // 2] + sums[width // 2 :]).reshape(split.shape[1:])
    stick_values = returned[:, :rows].reshape(owners, -1, 2, PLANES, bands, stick_count)
    picked = jnp.einsum(
        "dgpzbs,si->pdgzbi", stick_values, stick_hot, preferred_element_type=jnp.float32
    ).astype(jnp.bfloat16)
    picked = picked.reshape(2, grid_size, bands, -1)
    cosine_cols = jnp.einsum("zk,ki->zi", inverse[0], plane_hot, preferred_element_type=jnp.float32)
    sine_cols = jnp.einsum("zk,ki->zi", inverse[1], plane_hot, preferred_element_type=jnp.float32)
    pick_real = picked[0].astype(jnp.float32)
    pick_imag = picked[1].astype(jnp.float32)
    cosine_cols = cosine_cols[:, None]
    sine_cols = sine_cols[:, None]
    wave_real = jnp.sum(pick_real * cosine_cols - pick_imag * sine_cols, axis=0)
    wave_imag = jnp.sum(pick_real * sine_cols + pick_imag * cosine_cols, axis=0)
    real_out = wave_real + kinetic * orbitals[:, 0].astype(jnp.float32)
    imag_out = wave_imag + kinetic * orbitals[:, 1].astype(jnp.float32)
    applied = jnp.stack([real_out, imag_out], axis=1).astype(jnp.bfloat16)
    return (applied, intersection)


def per_device(mesh_bands, *arrays):
    orbitals, _, _, potential, _, previous = arrays
    slab_depth = potential.shape[0]
    bands = orbitals.shape[0]
    aligned = slab_depth % 8 == 0 and slab_depth % PLANES == 0
    aligned = aligned and LANES < potential.shape[1] <= 2 * LANES
    if aligned and PLANES * bands % 16 == 0 and arrays[2].shape[0] % 128 == 0:
        return fast_device(mesh_bands, *arrays)
    return general_device(*arrays)


def solution(mesh):
    return jax.shard_map(
        functools.partial(per_device, mesh.shape["band"]),
        mesh=mesh,
        in_specs=(
            P("band", None, "fft"),
            P("fft"),
            P("fft"),
            P("fft", None, None),
            P("band", None, "fft"),
            P("band", None, "fft"),
        ),
        out_specs=(P("band", None, "fft"), P(None, "fft", "band")),
        check_vma=False,
    )
```

```python
import functools
import math

import jax
import jax.numpy as jnp
import numpy as np
from jax import lax
from jax.experimental import pallas as pl
from jax.experimental.pallas import tpu as pltpu
from jax.sharding import PartitionSpec as P


def dft_table(length, sign_value, factor):
    positions = jnp.arange(length, dtype=jnp.int32)
    phase_step = positions[:, None] * positions[None, :] % length
    angle_value = phase_step.astype(jnp.float32) * (2.0 * math.pi / length)
    cosine = (jnp.cos(angle_value) * factor).astype(jnp.bfloat16)
    sine_part = (jnp.sin(angle_value) * (sign_value * factor)).astype(jnp.bfloat16)
    return (cosine, sine_part)


def apply_dft(real_in, imag_in, table, form):
    cosine, sine_part = table

    def product(operand, table_part):
        return jnp.einsum(form, operand, table_part, preferred_element_type=jnp.float32)

    real_out = product(real_in, cosine) - product(imag_in, sine_part)
    imag_out = product(real_in, sine_part) + product(imag_in, cosine)
    return (real_out, imag_out)


def packed(pair, axis_pos):
    return jnp.stack([pair[0].astype(jnp.bfloat16), pair[1].astype(jnp.bfloat16)], axis=axis_pos)


def frequency(values, grid_size):
    return jnp.where(values >= grid_size // 2, values - grid_size, values).astype(jnp.float32)


def one_hot_rows(indices, count):
    return (indices[None, :] == jnp.arange(count, dtype=jnp.int32)[:, None]).astype(jnp.bfloat16)


def general_device(orbitals, sphere_slot, stick_column, potential, subspace, previous):
    slab_depth = potential.shape[0]
    grid_size = potential.shape[1]
    stick_count = stick_column.shape[0]
    slab_cells = slab_depth * grid_size
    forward = dft_table(grid_size, 1.0, 1.0)
    inverse = dft_table(grid_size, -1.0, 1.0 / grid_size)
    plane_index = sphere_slot // stick_count
    stick_index = sphere_slot % stick_count
    plane_hot = one_hot_rows(plane_index, grid_size)
    stick_hot = one_hot_rows(stick_index, stick_count)
    stick_coords = jnp.stack([stick_column // grid_size, stick_column % grid_size]).astype(
        jnp.bfloat16
    )
    wave_coords = jnp.dot(stick_coords, stick_hot, preferred_element_type=jnp.float32)
    freq_z = frequency(plane_index, grid_size)
    freq_x = frequency(wave_coords[0].astype(jnp.int32), grid_size)
    freq_y = frequency(wave_coords[1].astype(jnp.int32), grid_size)
    kinetic = (freq_z * freq_z + freq_x * freq_x + freq_y * freq_y) * (
        2.0 / (grid_size * grid_size)
    )
    prev_real = previous[:, 0]
    prev_imag = previous[:, 1]
    sub_piece = lax.all_gather(subspace, "band", axis=0, tiled=True)
    sub_real = sub_piece[:, 0]
    sub_imag = sub_piece[:, 1]
    over_real = jnp.einsum(
        "jg,ig->ji", sub_real, prev_real, preferred_element_type=jnp.float32
    ) + jnp.einsum("jg,ig->ji", sub_imag, prev_imag, preferred_element_type=jnp.float32)
    over_imag = jnp.einsum(
        "jg,ig->ji", sub_real, prev_imag, preferred_element_type=jnp.float32
    ) - jnp.einsum("jg,ig->ji", sub_imag, prev_real, preferred_element_type=jnp.float32)
    partial_value = jnp.stack([over_real, over_imag])
    intersection = lax.psum_scatter(partial_value, "fft", scatter_dimension=1, tiled=True)
    stick_buffer = jnp.einsum(
        "bpi,zi,si->bpzs", orbitals, plane_hot, stick_hot, preferred_element_type=jnp.float32
    ).astype(jnp.bfloat16)

    def potential_work(along_y):
        along_x = apply_dft(along_y[0], along_y[1], forward, "zxy,xk->zky")
        weighted = packed((along_x[0] * potential, along_x[1] * potential), 0)
        back_x = packed(apply_dft(weighted[0], weighted[1], inverse, "zxy,xk->zky"), 0)
        return packed(apply_dft(back_x[0], back_x[1], inverse, "zxy,yk->zxk"), 0)

    along_z = packed(apply_dft(stick_buffer[:, 0], stick_buffer[:, 1], forward, "bzs,zk->bks"), 1)
    all_columns = lax.all_gather(stick_column, "fft", axis=0, tiled=True)
    owners = all_columns.shape[0] // stick_count
    block_columns = (all_columns % slab_cells).reshape(owners, stick_count)
    block_hot = (
        block_columns[:, :, None] == jnp.arange(slab_cells, dtype=jnp.int32)[None, None, :]
    ).astype(jnp.bfloat16)

    def stick_work(one_band):
        plane_depth = one_band.shape[1]
        split_band = one_band.reshape(2, plane_depth, owners, stick_count)
        plane_grid = jnp.einsum(
            "pzds,dsc->pzdc", split_band, block_hot, preferred_element_type=jnp.float32
        ).astype(jnp.bfloat16)
        plane_grid = plane_grid.reshape(2, plane_depth, grid_size, grid_size)
        along_y = packed(apply_dft(plane_grid[0], plane_grid[1], forward, "zxy,yk->zxk"), 0)
        back_y = potential_work(along_y)
        back_split = back_y.reshape(2, plane_depth, owners, slab_cells)
        picked = jnp.einsum(
            "pzdc,dsc->pzds", back_split, block_hot, preferred_element_type=jnp.float32
        ).astype(jnp.bfloat16)
        return picked.reshape(2, plane_depth, owners * stick_count)

    finished = lax.map(
        stick_work, lax.all_to_all(along_z, "fft", split_axis=2, concat_axis=3, tiled=True)
    )
    stick_values = lax.all_to_all(finished, "fft", split_axis=3, concat_axis=2, tiled=True)
    picked_sticks = jnp.einsum(
        "bpzs,si->bpzi", stick_values, stick_hot, preferred_element_type=jnp.float32
    ).astype(jnp.bfloat16)
    cosine_cols = jnp.einsum("zk,ki->zi", inverse[0], plane_hot, preferred_element_type=jnp.float32)
    sine_cols = jnp.einsum("zk,ki->zi", inverse[1], plane_hot, preferred_element_type=jnp.float32)
    pick_real = picked_sticks[:, 0].astype(jnp.float32)
    pick_imag = picked_sticks[:, 1].astype(jnp.float32)
    wave_real = jnp.sum(pick_real * cosine_cols[None] - pick_imag * sine_cols[None], axis=1)
    wave_imag = jnp.sum(pick_real * sine_cols[None] + pick_imag * cosine_cols[None], axis=1)
    real_out = wave_real + kinetic * orbitals[:, 0].astype(jnp.float32)
    imag_out = wave_imag + kinetic * orbitals[:, 1].astype(jnp.float32)
    applied = jnp.stack([real_out, imag_out], axis=1).astype(jnp.bfloat16)
    return (applied, intersection)


PLANES = 4
EXTRA = 16
LANES = 128


def phases(products, length):
    angle = (products % length).astype(np.float64) * (2.0 * np.pi / length)
    return np.cos(angle), np.sin(angle)


def line_tables(length):
    cosine, sine = phases(np.outer(np.arange(length), np.arange(length)), length)
    wide = -(-length // 128) * 128
    empty = np.zeros((length, wide - length))
    from_real = np.concatenate([cosine, empty, sine, empty], axis=1)
    from_imag = np.concatenate([-sine, empty, cosine, empty], axis=1)
    return jnp.asarray(np.stack([from_real, from_imag]), jnp.bfloat16)


def half_tables(length):
    half = np.arange(length // 2)
    tables = []
    for parity in (0, 1):
        cosine, sine = phases(np.outer(2 * half + parity, half), length)
        tables.append(np.block([[cosine, -sine], [sine, cosine]]))
    tables.extend([tables[0].T, tables[1].T])
    return jnp.asarray(np.stack(tables), jnp.bfloat16)


def column_tables(length):
    cosine, sine = phases(np.outer(np.arange(length), np.arange(length)), length)
    there = np.block([[cosine, -sine], [sine, cosine]])
    return jnp.asarray(there, jnp.bfloat16), jnp.asarray(there.T, jnp.bfloat16)


def plane_kernel(
    slab,
    sent_ref,
    pot_ref,
    line_ref,
    half_ref,
    extra_ref,
    back_ref,
    stick_ref,
    rows_ref,
    real_ref,
    imag_ref,
    after_real_ref,
    after_imag_ref,
    left_ref,
    right_ref,
    stage_ref,
    send_sem,
    recv_sem,
):
    owners, _, sticks = sent_ref.shape
    lines, size, _ = real_ref.shape
    half = size // 2
    wide = line_ref.shape[2] // 2
    groups = slab // PLANES
    part_rows = groups * lines
    me = lax.axis_index("fft")
    others = [lax.rem(me + shift, owners) for shift in range(1, owners)]
    scale = 1.0 / (size * size)

    def stick_mask(owner):
        coords = stick_ref[owner, 2 * part_rows : 2 * part_rows + EXTRA, :].astype(jnp.float32)
        local = lax.broadcasted_iota(jnp.int32, (slab, sticks), 0).astype(jnp.float32)
        return coords[0:1, :] == local

    def plane_group(group):
        first = pl.multiple_of(group * lines, lines)
        second = pl.multiple_of(part_rows + group * lines, lines)

        @pl.loop(0, owners, unroll=2)
        def _(owner):
            mask = stick_mask(owner)[None]
            spread = []
            for start in (first, second):
                values = stick_ref[owner, pl.ds(start, lines), :].astype(jnp.float32)
                spread.append(
                    jnp.where(mask, values[:, None, :], 0.0).reshape(lines * slab, sticks)
                )
            left = jnp.concatenate(spread, axis=1).astype(jnp.bfloat16)
            result = jnp.dot(left, rows_ref[owner], preferred_element_type=jnp.float32)
            place = pl.ds(pl.multiple_of(owner * slab, 8), slab)
            real_ref[:, place, :] = result[:, :size].reshape(lines, slab, size)
            imag_ref[:, place, :] = result[:, wide : wide + size].reshape(lines, slab, size)

        def one_plane(line, plane):
            real_low, real_high = real_ref[line, :half, :], real_ref[line, half:, :]
            imag_low, imag_high = imag_ref[line, :half, :], imag_ref[line, half:, :]
            total = jnp.concatenate([real_low + real_high, imag_low + imag_high], axis=0)
            differ = jnp.concatenate([real_low - real_high, imag_low - imag_high], axis=0)

            def there_and_back(values, parity):
                forward = jnp.dot(
                    half_ref[parity],
                    values.astype(jnp.bfloat16),
                    preferred_element_type=jnp.float32,
                )
                picks = pl.ds(parity, half, 2)
                local = jnp.concatenate(
                    [left_ref[plane, picks, :], right_ref[plane, picks, :][:, : size - LANES]], axis=1
                )
                weighted = jnp.concatenate([forward[:half] * local, forward[half:] * local], axis=0)
                return jnp.dot(
                    half_ref[2 + parity],
                    weighted.astype(jnp.bfloat16),
                    preferred_element_type=jnp.float32,
                )

            even = there_and_back(total, 0)
            odd = there_and_back(differ, 1)
            low, high = even + odd, even - odd
            after_real_ref[line, :half, :] = low[:half]
            after_imag_ref[line, :half, :] = low[half:]
            after_real_ref[line, half:, :] = high[:half]
            after_imag_ref[line, half:, :] = high[half:]

        bands = lines // PLANES

        @pl.loop(0, PLANES)
        def _(plane):
            whole_plane = group * PLANES + plane
            left_ref[plane] = pot_ref[whole_plane, :, :LANES]
            right_ref[plane, :, : size - LANES] = pot_ref[whole_plane, :, LANES:]
            for band in range(bands):
                one_plane(plane * bands + band, plane)

        @pl.loop(0, owners, unroll=2)
        def _(owner):
            mask = stick_mask(owner)[None]
            place = pl.ds(pl.multiple_of(owner * slab, 8), slab)
            real = after_real_ref[:, place, :].reshape(lines * slab, size).astype(jnp.bfloat16)
            imag = after_imag_ref[:, place, :].reshape(lines * slab, size).astype(jnp.bfloat16)
            across = (((1,), (1,)), ((), ()))
            result = lax.dot_general(
                real, rows_ref[owner, :, :size], across, preferred_element_type=jnp.float32
            ) + lax.dot_general(
                imag,
                rows_ref[owner, :, wide : wide + size],
                across,
                preferred_element_type=jnp.float32,
            )
            result = result.reshape(lines, slab, 2 * sticks)
            for part in range(2):
                chosen = result[:, :, part * sticks : (part + 1) * sticks]
                picked = jnp.sum(jnp.where(mask, chosen, 0.0), axis=1) * scale
                start = pl.multiple_of((2 * group + part) * lines, lines)
                stage_ref[owner, pl.ds(start, lines), :] = picked.astype(jnp.bfloat16)

    def rows_of(group):
        return pl.ds(pl.multiple_of(group * 2 * lines, 2 * lines), 2 * lines)

    def group_copy(group, place):
        return pltpu.make_async_remote_copy(
            src_ref=stage_ref.at[others[place], rows_of(group)],
            dst_ref=back_ref.at[me, rows_of(group)],
            send_sem=send_sem.at[group, place],
            recv_sem=recv_sem.at[group, place],
            device_id={"fft": others[place]},
            device_id_type=pl.DeviceIdType.MESH,
        )

    def extra_copy(place):
        return pltpu.make_async_remote_copy(
            src_ref=extra_ref.at[others[place]],
            dst_ref=back_ref.at[me, pl.ds(2 * part_rows, EXTRA)],
            send_sem=send_sem.at[groups, place],
            recv_sem=recv_sem.at[groups, place],
            device_id={"fft": others[place]},
            device_id_type=pl.DeviceIdType.MESH,
        )

    def stick_copy(place):
        return pltpu.make_async_remote_copy(
            src_ref=sent_ref.at[others[place]],
            dst_ref=stick_ref.at[me],
            send_sem=send_sem.at[groups + 1, place],
            recv_sem=recv_sem.at[groups + 1, place],
            device_id={"fft": others[place]},
            device_id_type=pl.DeviceIdType.MESH,
        )

    barrier = pltpu.get_barrier_semaphore()
    for other in others:
        pl.semaphore_signal(
            barrier, inc=1, device_id={"fft": other}, device_id_type=pl.DeviceIdType.MESH
        )

    pl.semaphore_wait(barrier, owners - 1)
    for place in range(owners - 1):
        stick_copy(place).start()
    for place in range(owners - 1):
        extra_copy(place).start()
    stick_ref[me] = sent_ref[me]
    for place in range(owners - 1):
        stick_copy(place).wait()

    @pl.loop(0, owners)
    def _(owner):
        coords = stick_ref[owner, 2 * part_rows : 2 * part_rows + EXTRA, :].astype(jnp.float32)
        cells = lax.broadcasted_iota(jnp.int32, (size, sticks), 0).astype(jnp.float32)
        hot = jnp.where(coords[1:2, :] == cells, 1.0, 0.0).astype(jnp.bfloat16)
        for part in range(2):
            rows = lax.dot_general(
                hot,
                line_ref[part],
                (((0,), (0,)), ((), ())),
                preferred_element_type=jnp.float32,
            )
            rows_ref[owner, part * sticks : (part + 1) * sticks, :] = rows.astype(jnp.bfloat16)

    @pl.loop(0, groups)
    def _(group):
        plane_group(group)
        for place in range(owners - 1):
            group_copy(group, place).start()

    back_ref[me, : 2 * part_rows, :] = stage_ref[me]
    back_ref[me, 2 * part_rows :, :] = extra_ref[me]
    for place in range(owners - 1):
        extra_copy(place).wait()

    @pl.loop(0, groups)
    def _(group):
        for place in range(owners - 1):
            group_copy(group, place).wait()


def plane_work(sent, potential, extra, bands):
    owners, _, sticks = sent.shape
    slab, size, _ = potential.shape
    lines = PLANES * bands
    groups = slab // PLANES
    lines_table = line_tables(size)
    halves = half_tables(size)
    wide = lines_table.shape[2]
    rows = 2 * slab * bands
    in_vmem = pl.BlockSpec(memory_space=pltpu.VMEM)
    grid_part = pltpu.VMEM((lines, size, size), jnp.float32)
    return pl.pallas_call(
        functools.partial(plane_kernel, slab),
        out_shape=jax.ShapeDtypeStruct((owners, rows + EXTRA, sticks), jnp.bfloat16),
        in_specs=[in_vmem] * 5,
        out_specs=in_vmem,
        scratch_shapes=[
            pltpu.VMEM((owners, rows + EXTRA, sticks), jnp.bfloat16),
            pltpu.VMEM((owners, 2 * sticks, wide), jnp.bfloat16),
            grid_part,
            grid_part,
            grid_part,
            grid_part,
            pltpu.VMEM((PLANES, size, LANES), jnp.float32),
            pltpu.VMEM((PLANES, size, LANES), jnp.float32),
            pltpu.VMEM((owners, rows, sticks), jnp.bfloat16),
            pltpu.SemaphoreType.DMA((groups + 2, owners - 1)),
            pltpu.SemaphoreType.DMA((groups + 2, owners - 1)),
        ],
        compiler_params=pltpu.CompilerParams(
            collective_id=0, has_side_effects=True, vmem_limit_bytes=48 * 1024 * 1024
        ),
        cost_estimate=pl.CostEstimate(
            flops=40 * 10**9, bytes_accessed=8 * 10**6, transcendentals=0
        ),
    )(sent, potential, lines_table, halves, extra)


def gathered_bands(array, mesh_bands):
    here = lax.axis_index("band")
    blocks = [array]
    for shift in range(1, mesh_bands):
        pairs = [((src + shift) % mesh_bands, src) for src in range(mesh_bands)]
        blocks.append(lax.ppermute(array, "band", pairs))
    return blocks, here


def overlaps(subspace, previous, mesh_bands, owners):
    blocks, here = gathered_bands(subspace, mesh_bands)
    prev_real, prev_imag = previous[:, 0], previous[:, 1]
    right = jnp.concatenate(
        [
            jnp.concatenate([prev_real, prev_imag], axis=1),
            jnp.concatenate([prev_imag, -prev_real], axis=1),
        ],
        axis=0,
    )
    partials = []
    for block in blocks:
        partials.append(
            jnp.einsum(
                "jg,ig->ji",
                block.reshape(block.shape[0], -1),
                right,
                preferred_element_type=jnp.float32,
            )
        )
    twice = jnp.concatenate(partials + partials, axis=0)
    count = twice.shape[0] // 2
    start = (count - here * subspace.shape[0]) % count
    ordered = lax.dynamic_slice_in_dim(twice, start, count, axis=0)
    split = ordered.reshape(owners, count // owners, 2, previous.shape[0])
    return split.transpose(0, 2, 1, 3)


def fast_device(mesh_bands, orbitals, sphere_slot, stick_column, potential, subspace, previous):
    slab_depth, grid_size, _ = potential.shape
    stick_count = stick_column.shape[0]
    owners = grid_size // slab_depth
    bands = orbitals.shape[0]
    plane_index = sphere_slot // stick_count
    stick_index = sphere_slot % stick_count
    plane_hot = one_hot_rows(plane_index, grid_size)
    stick_hot = one_hot_rows(stick_index, stick_count)
    stick_x = stick_column // grid_size
    stick_y = stick_column % grid_size
    stick_coords = jnp.stack([stick_x, stick_y]).astype(jnp.bfloat16)
    wave_coords = jnp.dot(stick_coords, stick_hot, preferred_element_type=jnp.float32)
    freq_z = frequency(plane_index, grid_size)
    freq_x = frequency(wave_coords[0].astype(jnp.int32), grid_size)
    freq_y = frequency(wave_coords[1].astype(jnp.int32), grid_size)
    kinetic = (freq_z * freq_z + freq_x * freq_x + freq_y * freq_y) * (
        2.0 / (grid_size * grid_size)
    )
    local_x = stick_x - lax.axis_index("fft") * slab_depth
    coords = jnp.stack([local_x, stick_y]).astype(jnp.bfloat16)
    coords = jnp.pad(coords, ((0, EXTRA - 2), (0, 0)))
    coords = jnp.broadcast_to(coords[None], (owners, EXTRA, stick_count))
    stick_buffer = jnp.einsum(
        "bpi,zi,si->pzbs", orbitals, plane_hot, stick_hot, preferred_element_type=jnp.float32
    ).astype(jnp.bfloat16)
    forward, backward = column_tables(grid_size)
    along_z = jnp.dot(
        forward,
        stick_buffer.reshape(2 * grid_size, bands * stick_count),
        preferred_element_type=jnp.float32,
    ).astype(jnp.bfloat16)
    along_z = along_z.reshape(2, owners, slab_depth * bands, stick_count)
    pieces = [along_z[0], along_z[1]]
    sent = jnp.concatenate(pieces + [coords], axis=1)
    split = overlaps(subspace, previous, mesh_bands, owners)
    flat = split.reshape(owners, 1, -1)
    high = lax.reduce_precision(flat, 8, 7)
    low = lax.reduce_precision(flat - high, 8, 7)
    both = jnp.concatenate([high, low], axis=2).astype(jnp.bfloat16)
    width = both.shape[2]
    lanes = -(-width // stick_count) * stick_count
    both = jnp.pad(both, ((0, 0), (0, 0), (0, lanes - width)))
    both = both.reshape(owners, -1, stick_count)
    both = jnp.pad(both, ((0, 0), (0, EXTRA - both.shape[1]), (0, 0)))
    returned = plane_work(sent, potential, both, bands)
    rows = 2 * slab_depth * bands
    sums = returned[:, rows:].reshape(owners, -1)[:, :width].astype(jnp.float32)
    sums = jnp.sum(sums, axis=0)
    intersection = (sums[: width // 2] + sums[width // 2 :]).reshape(split.shape[1:])
    stick_values = returned[:, :rows].reshape(owners, -1, 2, PLANES, bands * stick_count)
    stick_values = stick_values.transpose(2, 0, 1, 3, 4).reshape(2 * grid_size, -1)
    columns = jnp.dot(backward, stick_values, preferred_element_type=jnp.float32)
    columns = (columns * (1.0 / grid_size)).astype(jnp.bfloat16)
    columns = columns.reshape(2, grid_size, bands, stick_count)
    picked = jnp.einsum(
        "pzbs,si->pzbi", columns, stick_hot, preferred_element_type=jnp.float32
    ).astype(jnp.bfloat16)
    levels = jnp.arange(grid_size, dtype=jnp.int32)[:, None]
    here = (plane_index[None, :] == levels)[None, :, None, :]
    waves = jnp.sum(jnp.where(here, picked.astype(jnp.float32), 0.0), axis=1)
    wave_real, wave_imag = waves[0], waves[1]
    real_out = wave_real + kinetic * orbitals[:, 0].astype(jnp.float32)
    imag_out = wave_imag + kinetic * orbitals[:, 1].astype(jnp.float32)
    applied = jnp.stack([real_out, imag_out], axis=1).astype(jnp.bfloat16)
    return (applied, intersection)


def per_device(mesh_bands, *arrays):
    orbitals, _, _, potential, _, previous = arrays
    slab_depth = potential.shape[0]
    bands = orbitals.shape[0]
    aligned = slab_depth % 8 == 0 and slab_depth % PLANES == 0
    aligned = aligned and LANES < potential.shape[1] <= 2 * LANES
    if aligned and PLANES * bands % 16 == 0 and arrays[2].shape[0] % 128 == 0:
        return fast_device(mesh_bands, *arrays)
    return general_device(*arrays)


def solution(mesh):
    return jax.shard_map(
        functools.partial(per_device, mesh.shape["band"]),
        mesh=mesh,
        in_specs=(
            P("band", None, "fft"),
            P("fft"),
            P("fft"),
            P("fft", None, None),
            P("band", None, "fft"),
            P("band", None, "fft"),
        ),
        out_specs=(P("band", None, "fft"), P(None, "fft", "band")),
        check_vma=False,
    )
```
